768 devices in a mesh: section: 32 (over y, z_hi), tensor: 4 (over x), dp: 6 (over z_lo, core).
Axes of the slice: x: 4, y: 8, z: 12 (z_hi: 4, z_lo: 3; z = z_hi * 3 + z_lo), core: 2. Of those that a mesh axis runs over, the one named last changes fastest.
Arguments:
- forward_rows: bfloat16 [32, 6, 192, 8192], P('section', 'dp', None, 'tensor'), may hold values from -6 to 6
- saved_rows: bfloat16 [32, 6, 192, 8192], P('section', 'dp', None, 'tensor'), may hold values from -40.5 to 40.5
- output_grad: bfloat16 [32, 6, 192, 8192], P('section', 'dp', None, 'tensor'), may hold values from -1.27 to 1.27
- lengths: int32 [32, 6, 2], P('section', 'dp'), may hold values from 1 to 96
- norm_gain: bfloat16 [32, 8192], P('section', 'tensor'), may hold values from 0.5 to 1.5
- down_map: bfloat16 [32, 192, 8192], P('section', None, 'tensor'), may hold values from -0.067396115 to 0.067396115
- up_map: bfloat16 [32, 192, 8192], P('section', None, 'tensor'), may hold values from -1.0625 to 1.0625
Outputs:
- next_inputs: bfloat16 [32, 6, 192, 8192], P('section', 'dp', None, 'tensor')
- next_grads: bfloat16 [32, 6, 192, 8192], P('section', 'dp', None, 'tensor')
- grad_down: bfloat16 [32, 192, 8192], P('section', 'dp', 'tensor')
- grad_up: bfloat16 [32, 192, 8192], P('section', 'dp', 'tensor')
The draws below stay inside these ranges and needn't reach their ends.
All inputs are finite; a program needn't handle non-finite values.
Results may differ from the reference program's by a relative error of at most 0.02.
Values may be sent and summed in bfloat16 or wider, within the bound.
A program may use at most 32 MiB of HBM per device.

```python
import jax
import jax.numpy as jnp
from jax import lax

D = 8192
R = 192
ROWS = 192
SEQ = 96
N_SECTION = 32
N_DP = 6


def shared_rows(key):
    base = jax.random.fold_in(key, 11)
    shape = (N_SECTION, N_DP, ROWS, D)
    return jnp.clip(jax.random.normal(base, shape, jnp.float32), -6.0, 6.0)


def draw_saved_rows(key, part):
    values = shared_rows(key)
    return values.astype(jnp.bfloat16)


def draw_output_grad(key, part):
    shared = shared_rows(key)
    noise = jax.random.normal(jax.random.fold_in(key, 13), shared.shape, jnp.float32)
    mixed = 0.8 * shared + 0.6 * jnp.clip(noise, -6.0, 6.0)
    return (0.15 * mixed).astype(jnp.bfloat16)


def map_values(key, salt):
    base = jax.random.fold_in(key, salt)
    shape = (N_SECTION, R, D)
    return jnp.clip(jax.random.normal(base, shape, jnp.float32), -6.0, 6.0)


def draw_down_map(key, part):
    return (map_values(key, 21) * D ** (-0.5)).astype(jnp.bfloat16)


def draw_up_map(key, part):
    shared = map_values(key, 21)
    own_part = map_values(key, 22)
    mixed = 0.8 * shared + 0.6 * own_part
    return (mixed * (R // 3) ** (-0.5)).astype(jnp.bfloat16)


def place_ends(result, key, smallest, top_value):
    extent = result.shape
    place = [jax.random.randint(jax.random.fold_in(key, axis), (), 0, extent[axis]) for axis in range(len(extent))]
    result = result.at[tuple(place)].set(smallest)
    longest = extent.index(max(extent))
    place[longest] = (place[longest] + 1) % extent[longest]
    return result.at[tuple(place)].set(top_value)


def level_of(rng, extent, split, smallest, high):
    gain, own = 1.0, jax.random.fold_in(rng, 6)
    for dim, parts in split:
        draws = jnp.exp(jax.random.uniform(jax.random.fold_in(own, dim), (parts,), jnp.float32, smallest / len(split), high / len(split)))
        gain = gain * jnp.repeat(draws, extent[dim] // parts).reshape([-1 if axis == dim else 1 for axis in range(len(extent))])
    return gain


def normal_values(stream_key, dims, scale, most, pieces=(), held_as=jnp.bfloat16):
    factor_of = level_of(stream_key, dims, pieces, -0.22, 0.18) if pieces else 1.0
    values = jax.random.normal(stream_key, dims, jnp.float32) * scale * factor_of
    return jnp.minimum(jnp.maximum(values, -most), most).astype(held_as)


def setup_inputs(seed: int = 0) -> dict:
    seeds = jax.random.split(jax.random.key(seed), 8)
    forward_rows = normal_values(seeds[0], (N_SECTION, N_DP, ROWS, D), 1.0, 6.0, ((0, 32), (1, 6), (3, 4)))
    saved_rows = draw_saved_rows(jax.random.fold_in(seeds[7], 71), 0)
    output_grad = draw_output_grad(jax.random.fold_in(seeds[7], 71), 0)
    lengths = place_ends(jax.random.randint(seeds[3], (N_SECTION, N_DP, 2), 1, SEQ + 1), jax.random.fold_in(seeds[3], 1), 1, SEQ).astype(jnp.int32)
    norm_gain = jnp.clip(1.0 + 0.1 * jax.random.normal(seeds[4], (N_SECTION, D), jnp.float32), 0.5, 1.5).astype(jnp.bfloat16)
    down_map = draw_down_map(jax.random.fold_in(seeds[7], 71), 0)
    up_map = draw_up_map(jax.random.fold_in(seeds[7], 71), 0)
    return dict(forward_rows=forward_rows, saved_rows=saved_rows, output_grad=output_grad, lengths=lengths, norm_gain=norm_gain, down_map=down_map, up_map=up_map)


EPSILON = 1e-05

def contract_last(left_side, right_side):
    return lax.dot_general(left_side, right_side, (((1,), (1,)), ((), ())), preferred_element_type=jnp.float32)

def contract_rows(left_side, right_side):
    return lax.dot_general(left_side, right_side, (((0,), (0,)), ((), ())), preferred_element_type=jnp.float32)

def silu_slope(values):
    gate_value = jax.nn.sigmoid(values)
    return gate_value * (1.0 + values * (1.0 - gate_value))

def norm_rows(row_block, gain_cols):
    values = row_block.astype(jnp.float32)
    scale = lax.rsqrt(lax.optimization_barrier(jnp.mean(values * values, axis=1, keepdims=True)) + EPSILON)
    return (values, scale, (values * scale * gain_cols).astype(jnp.bfloat16))

def group_tick(forward_block, saved_block, incoming, seq_lengths, gain_cols, down_rows, up_rows):
    forward_values, forward_scale, forward_normed = norm_rows(forward_block, gain_cols)
    forward_act = jax.nn.silu(contract_last(forward_normed, down_rows)).astype(jnp.bfloat16)
    forward_out = (forward_values + jnp.dot(forward_act, up_rows, preferred_element_type=jnp.float32)).astype(jnp.bfloat16)
    position = jnp.arange(ROWS, dtype=jnp.int32)
    length_limit = jnp.where(position // SEQ == 0, seq_lengths[0], seq_lengths[1])
    keep_rows = position % SEQ < length_limit
    kept_grad = jnp.where(keep_rows[:, None], incoming, jnp.zeros_like(incoming))
    saved_values, saved_scale, saved_normed = norm_rows(saved_block, gain_cols)
    saved_rank = contract_last(saved_normed, down_rows)
    saved_act = jax.nn.silu(saved_rank).astype(jnp.bfloat16)
    rank_slope = contract_last(kept_grad, up_rows)
    back_rank = (rank_slope * silu_slope(saved_rank)).astype(jnp.bfloat16)
    back_normed = jnp.dot(back_rank, down_rows, preferred_element_type=jnp.float32)
    weighted = gain_cols * back_normed
    correction = lax.optimization_barrier(jnp.mean(saved_values * weighted, axis=1, keepdims=True))
    scale_cube = saved_scale * saved_scale * saved_scale
    grad_rows = (kept_grad.astype(jnp.float32) + saved_scale * weighted - saved_values * scale_cube * correction).astype(jnp.bfloat16)
    down_part = contract_rows(back_rank, saved_normed).astype(jnp.bfloat16)
    up_part = contract_rows(saved_act, kept_grad).astype(jnp.bfloat16)
    return (forward_out, grad_rows, down_part, up_part)

def section_tick(packed):
    forward_block, saved_block, incoming, seq_lengths, gain_row, down_rows, up_rows = packed
    gain_cols = gain_row.astype(jnp.float32)
    group_map = jax.vmap(group_tick, in_axes=(0, 0, 0, 0, None, None, None))
    forward_out, grad_rows, down_part, up_part = group_map(forward_block, saved_block, incoming, seq_lengths, gain_cols, down_rows, up_rows)
    down_part = lax.optimization_barrier(down_part)
    up_part = lax.optimization_barrier(up_part)
    mean_weight = 1.0 / N_DP
    grad_down = (lax.optimization_barrier(jnp.sum(down_part.astype(jnp.float32), axis=0)) * mean_weight).astype(jnp.bfloat16)
    grad_up = (lax.optimization_barrier(jnp.sum(up_part.astype(jnp.float32), axis=0)) * mean_weight).astype(jnp.bfloat16)
    return (forward_out, grad_rows, grad_down, grad_up)

def reference(forward_rows, saved_rows, output_grad, lengths, norm_gain, down_map, up_map):
    forward_out, grad_rows, grad_down, grad_up = lax.map(section_tick, (forward_rows, saved_rows, output_grad, lengths, norm_gain, down_map, up_map))
    next_inputs = jnp.concatenate([jnp.zeros_like(forward_out[:1]), forward_out[:-1]], axis=0)
    next_grads = jnp.concatenate([grad_rows[1:], jnp.zeros_like(grad_rows[:1])], axis=0)
    return (next_inputs, next_grads, grad_down, grad_up)
```

```python
import functools

import jax
import jax.numpy as jnp
from jax import lax
from jax.experimental import pallas as pl
from jax.experimental.pallas import tpu as pltpu
from jax.sharding import PartitionSpec as P

EPSILON = 1e-05
MESH = pl.DeviceIdType.MESH
CHUNKS = ((0, 16), (16, 32), (48, 64), (112, 80))
TILE = 256
ROW_BLOCK = 16


def remote(src, dst, send_sem, recv_sem, target):
    return pltpu.make_async_remote_copy(
        src_ref=src, dst_ref=dst, send_sem=send_sem, recv_sem=recv_sem, device_id=target, device_id_type=MESH
    )


def contract(left, right, dims):
    return lax.dot_general(left, right, ((dims[:1], dims[1:]), ((), ())), preferred_element_type=jnp.float32)


def kernel(
    n_section, n_tensor, n_dp,
    lens, gain, f_hbm, s_hbm, g_hbm, d_hbm, u_hbm,
    next_f, next_g, grad_down, grad_up,
    fwd, saved, kept, down, up, squares, fwd_out, back_out, own, others, sact_all, back_all,
    parts, from_core, chip_sum, from_chip, mean_out,
    load_sem, x_send, x_recv, f_send, f_recv, b_send, b_recv, c_send, c_recv, z_send, z_recv, out_sem,
):
    rows, cols = fwd.shape
    units = down.shape[0]
    width = cols * n_tensor
    sec, ten, dp = lax.axis_index("section"), lax.axis_index("tensor"), lax.axis_index("dp")
    n_z = n_dp // 2
    z, core = dp // 2, dp % 2
    has_next, has_prev = sec < n_section - 1, sec > 0

    loads = []
    for i, (src, dst) in enumerate(((d_hbm, down), (s_hbm, saved), (u_hbm, up), (g_hbm, kept), (f_hbm, fwd))):
        loads.append(pltpu.make_async_copy(src, dst, load_sem.at[i]))
        loads[-1].start()
    down_load, saved_load, up_load, kept_load, fwd_load = loads

    x_peers = [{"tensor": lax.rem(ten + k, n_tensor)} for k in range(1, n_tensor)]
    core_peer = {"dp": z * 2 + 1 - core}
    z_peers = [{"dp": lax.rem(z + k, n_z) * 2 + core} for k in range(1, n_z)]
    barrier = pltpu.get_barrier_semaphore()
    for peer in (*x_peers, core_peer, *z_peers):
        pl.semaphore_signal(barrier, inc=1, device_id=peer, device_id_type=MESH)

    @pl.when(has_next)
    def _():
        pl.semaphore_signal(barrier, inc=1, device_id={"section": sec + 1}, device_id_type=MESH)

    @pl.when(has_prev)
    def _():
        pl.semaphore_signal(barrier, inc=1, device_id={"section": sec - 1}, device_id_type=MESH)

    def row_blocks(body):
        def step(i, carry):
            body(pl.ds(pl.multiple_of(i * ROW_BLOCK, ROW_BLOCK), ROW_BLOCK))
            return carry

        lax.fori_loop(0, rows // ROW_BLOCK, step, 0, unroll=True)

    def col_tiles(body):
        def step(i, carry):
            body(pl.ds(pl.multiple_of(i * TILE, TILE), TILE))
            return carry

        lax.fori_loop(0, cols // TILE, step, 0, unroll=2)

    gain_row = gain[...].astype(jnp.float32)

    def scale_down(r):
        down[r, :] = (down[r, :].astype(jnp.float32) * gain_row).astype(jnp.bfloat16)

    def squares_of(ref):
        def body(r):
            values = ref[r, :].astype(jnp.float32)
            values = values * values
            total = values[:, :128]
            for j in range(1, cols // 128):
                total = total + values[:, j * 128 : (j + 1) * 128]
            squares[r, :] = total

        row_blocks(body)
        return jnp.sum(squares[...], axis=1, keepdims=True)

    def place(which, part, total):
        part = part.astype(jnp.bfloat16)
        for r0, n in CHUNKS:
            at = 3 * r0 + which * n
            own[at : at + n, :units] = part[r0 : r0 + n]
            if total is not None:
                own[at : at + n, units:] = jnp.broadcast_to(total[r0 : r0 + n].astype(jnp.bfloat16), (n, 256 - units))

    down_load.wait()
    row_blocks(scale_down)
    saved_load.wait()
    place(1, contract(saved[...], down[...], (1, 1)), squares_of(saved))

    kept_load.wait()

    def mask_rows(r):
        row = r.start + lax.broadcasted_iota(jnp.int32, (ROW_BLOCK, cols), 0)
        half = rows // 2
        second = row >= half
        position = jnp.where(second, row - half, row)
        limit = jnp.where(second, lens[1], lens[0])
        values = kept[r, :].astype(jnp.float32)
        kept[r, :] = jnp.where(position < limit, values, 0.0).astype(jnp.bfloat16)

    row_blocks(mask_rows)
    up_load.wait()
    place(2, contract(kept[...], up[...], (1, 1)), None)
    fwd_load.wait()
    place(0, contract(fwd[...], down[...], (1, 1)), squares_of(fwd))

    sections = (sec + n_section - 1) // n_section + (2 * n_section - 2 - sec) // n_section
    pl.semaphore_wait(barrier, n_tensor - 1 + 1 + n_z - 1 + sections)

    x_copies = []
    for c, (r0, n) in enumerate(CHUNKS):
        at = pl.ds(3 * r0, 3 * n)
        x_copies.append([
            remote(own.at[at], others.at[k, at], x_send.at[c, k], x_recv.at[c, k], x_peers[k])
            for k in range(n_tensor - 1)
        ])
        for copy in x_copies[-1]:
            copy.start()

    f_copies, b_copies = [], []
    for c, (r0, n) in enumerate(CHUNKS):
        for copy in x_copies[c]:
            copy.wait_recv()

        def summed(which):
            at = pl.ds(3 * r0 + which * n, n)
            total = own[at, :].astype(jnp.float32)
            for k in range(n_tensor - 1):
                total = total + others[k, at, :].astype(jnp.float32)
            return total

        r = pl.ds(r0, n)
        saved_total = summed(1)
        saved_scale = lax.rsqrt(saved_total[:, units : units + 1] / width + EPSILON)
        saved_rank = saved_total[:, :units] * saved_scale
        gate = jax.nn.sigmoid(saved_rank)
        sact_all[r, :] = (saved_rank * gate).astype(jnp.bfloat16)
        back = summed(2)[:, :units] * (gate * (1.0 + saved_rank * (1.0 - gate)))
        pull = saved_scale * saved_scale * (jnp.sum(back * saved_rank, axis=1, keepdims=True) / width)
        back = (back * saved_scale).astype(jnp.bfloat16)
        back_all[r, :] = back
        fwd_total = summed(0)
        fwd_scale = lax.rsqrt(fwd_total[:, units : units + 1] / width + EPSILON)
        act = jax.nn.silu(fwd_total[:, :units] * fwd_scale).astype(jnp.bfloat16)

        def back_tile(t):
            weighted = contract(back, down[:, t], (1, 0))
            values = kept[r, t].astype(jnp.float32) + weighted - saved[r, t].astype(jnp.float32) * pull
            back_out[r, t] = values.astype(jnp.bfloat16)

        col_tiles(back_tile)
        b_copies.append(remote(back_out.at[r], next_g.at[r], b_send.at[c], b_recv.at[c], {"section": sec - 1}))

        @pl.when(has_prev)
        def _():
            b_copies[c].start()

        def fwd_tile(t):
            raised = contract(act, up[:, t], (1, 0))
            fwd_out[r, t] = (fwd[r, t].astype(jnp.float32) + raised).astype(jnp.bfloat16)

        col_tiles(fwd_tile)
        f_copies.append(remote(fwd_out.at[r], next_f.at[r], f_send.at[c], f_recv.at[c], {"section": sec + 1}))

        @pl.when(has_next)
        def _():
            f_copies[c].start()

    def part_tile(t):
        share = units // n_dp
        down_part = (contract(back_all[...], saved[:, t], (0, 0)) * gain[:, t].astype(jnp.float32)).astype(jnp.bfloat16)
        up_part = contract(sact_all[...], kept[:, t], (0, 0)).astype(jnp.bfloat16)
        for i in range(n_dp):
            at = slice(i * share, (i + 1) * share)
            parts[i % 2, i // 2, 0, :, t] = down_part[at]
            parts[i % 2, i // 2, 1, :, t] = up_part[at]

    col_tiles(part_tile)
    order = [lax.rem(z + k, n_z) for k in (*range(1, n_z), 0)]
    c_copies = []
    for i, at in enumerate(order):
        c_copies.append(remote(parts.at[1 - core, at], from_core.at[i], c_send.at[i], c_recv.at[i], core_peer))
        c_copies[-1].start()
    z_copies = []
    for i, at in enumerate(order):
        c_copies[i].wait_recv()

        def add(t):
            for a in range(2):
                chip_sum[i, a, :, t] = (
                    parts[core, at, a, :, t].astype(jnp.float32) + from_core[i, a, :, t].astype(jnp.float32)
                ).astype(jnp.bfloat16)

        col_tiles(add)
        if i < n_z - 1:
            z_copies.append(remote(chip_sum.at[i], from_chip.at[i], z_send.at[i], z_recv.at[i], z_peers[i]))
            z_copies[-1].start()
    for copy in z_copies:
        copy.wait_recv()

    def finish(t):
        for a in range(2):
            total = chip_sum[n_z - 1, a, :, t].astype(jnp.float32)
            for i in range(n_z - 1):
                total = total + from_chip[i, a, :, t].astype(jnp.float32)
            mean_out[a, :, t] = (total * (1.0 / n_dp)).astype(jnp.bfloat16)

    col_tiles(finish)
    outs = [
        pltpu.make_async_copy(mean_out.at[a], dst, out_sem.at[a]) for a, dst in enumerate((grad_down, grad_up))
    ]
    for copy in outs:
        copy.start()

    for copies in x_copies:
        for copy in copies:
            copy.wait_send()
    for copy in (*c_copies, *z_copies):
        copy.wait_send()
    for c in range(len(CHUNKS)):
        @pl.when(has_prev)
        def _():
            b_copies[c].wait_send()
            f_copies[c].wait_recv()

        @pl.when(has_next)
        def _():
            f_copies[c].wait_send()
            b_copies[c].wait_recv()
    for copy in outs:
        copy.wait()


def solution(mesh):
    n_section, n_tensor, n_dp = (mesh.shape[a] for a in ("section", "tensor", "dp"))
    n_z = n_dp // 2

    def shards(forward_rows, saved_rows, output_grad, lengths, norm_gain, down_map, up_map):
        rows, cols = forward_rows.shape[2:]
        units = down_map.shape[1]
        share = units // n_dp
        n = len(CHUNKS)
        bf16 = jnp.bfloat16
        anywhere = pl.BlockSpec(memory_space=pl.ANY)
        dma = pltpu.SemaphoreType.DMA
        got_f, got_g, grad_down, grad_up = pl.pallas_call(
            functools.partial(kernel, n_section, n_tensor, n_dp),
            out_shape=(
                jax.ShapeDtypeStruct((rows, cols), bf16),
                jax.ShapeDtypeStruct((rows, cols), bf16),
                jax.ShapeDtypeStruct((share, cols), bf16),
                jax.ShapeDtypeStruct((share, cols), bf16),
            ),
            in_specs=[
                pl.BlockSpec(memory_space=pltpu.SMEM),
                pl.BlockSpec(memory_space=pltpu.VMEM),
                *[anywhere] * 5,
            ],
            out_specs=(anywhere,) * 4,
            scratch_shapes=[
                *[pltpu.VMEM((rows, cols), bf16)] * 3,
                *[pltpu.VMEM((units, cols), bf16)] * 2,
                pltpu.VMEM((rows, 128), jnp.float32),
                *[pltpu.VMEM((rows, cols), bf16)] * 2,
                pltpu.VMEM((3 * rows, 256), bf16),
                pltpu.VMEM((n_tensor - 1, 3 * rows, 256), bf16),
                *[pltpu.VMEM((rows, units), bf16)] * 2,
                pltpu.VMEM((2, n_z, 2, share, cols), bf16),
                pltpu.VMEM((n_z, 2, share, cols), bf16),
                pltpu.VMEM((n_z, 2, share, cols), bf16),
                pltpu.VMEM((n_z - 1, 2, share, cols), bf16),
                pltpu.VMEM((2, share, cols), bf16),
                dma((5,)),
                *[dma((n, n_tensor - 1))] * 2,
                *[dma((n,))] * 4,
                *[dma((n_z,))] * 2,
                *[dma((n_z - 1,))] * 2,
                dma((2,)),
            ],
            compiler_params=pltpu.CompilerParams(
                collective_id=0, has_side_effects=True, vmem_limit_bytes=48 * 1024 * 1024
            ),
        )(
            lengths[0, 0],
            norm_gain,
            forward_rows[0, 0],
            saved_rows[0, 0],
            output_grad[0, 0],
            down_map[0],
            up_map[0],
        )
        sec = lax.axis_index("section")
        next_inputs = jnp.where(sec > 0, got_f, jnp.zeros_like(got_f))
        next_grads = jnp.where(sec < n_section - 1, got_g, jnp.zeros_like(got_g))
        return next_inputs[None, None], next_grads[None, None], grad_down[None], grad_up[None]

    wide = P("section", "dp", None, "tensor")
    return jax.shard_map(
        shards,
        mesh=mesh,
        in_specs=(
            wide, wide, wide, P("section", "dp", None), P("section", "tensor"),
            P("section", None, "tensor"), P("section", None, "tensor"),
        ),
        out_specs=(wide, wide, P("section", "dp", "tensor"), P("section", "dp", "tensor")),
        check_vma=False,
    )
```

```python
import functools

import jax
import jax.numpy as jnp
from jax import lax
from jax.experimental import pallas as pl
from jax.experimental.pallas import tpu as pltpu
from jax.sharding import PartitionSpec as P

EPSILON = 1e-05
MESH = pl.DeviceIdType.MESH
CHUNKS = ((0, 16), (16, 32), (48, 64), (112, 80))
TILE = 256
ROW_BLOCK = 16
PIECES = 4


def remote(src, dst, send_sem, recv_sem, target):
    return pltpu.make_async_remote_copy(
        src_ref=src, dst_ref=dst, send_sem=send_sem, recv_sem=recv_sem, device_id=target, device_id_type=MESH
    )


def contract(left, right, dims):
    return lax.dot_general(left, right, ((dims[:1], dims[1:]), ((), ())), preferred_element_type=jnp.float32)


def kernel(
    n_section, n_tensor, n_dp,
    lens_hbm, gain_hbm, f_hbm, s_hbm, g_hbm, d_hbm, u_hbm,
    next_f, next_g, grad_down, grad_up,
    fwd, saved, kept, down, up, squares, fwd_out, back_out, own, others, sact_all, back_all,
    parts, from_core, chip_sum, from_chip,
    lens, gain, small_sem, load_sem, x_send, x_recv, f_send, f_recv, b_send, b_recv, c_send, c_recv, z_send, z_recv,
):
    rows, cols = fwd.shape
    units = down.shape[0]
    width = cols * n_tensor
    sec, ten, dp = lax.axis_index("section"), lax.axis_index("tensor"), lax.axis_index("dp")
    n_z = n_dp // 2
    z, core = dp // 2, dp % 2
    has_next, has_prev = sec < n_section - 1, sec > 0

    lens_load = pltpu.make_async_copy(lens_hbm, lens, small_sem.at[0])
    gain_load = pltpu.make_async_copy(gain_hbm, gain, small_sem.at[1])
    gain_load.start()
    lens_load.start()
    loads = []
    for i, (src, dst) in enumerate(((d_hbm, down), (s_hbm, saved), (u_hbm, up), (g_hbm, kept), (f_hbm, fwd))):
        loads.append([])
        for j in range(PIECES):
            at = pl.ds(j * (rows // PIECES), rows // PIECES)
            loads[-1].append(pltpu.make_async_copy(src.at[at], dst.at[at], load_sem.at[i, j]))
            loads[-1][-1].start()
    down_load, saved_load, up_load, kept_load, fwd_load = loads

    def loaded(pieces):
        for piece in pieces:
            piece.wait()

    x_peers = [{"tensor": lax.rem(ten + k, n_tensor)} for k in range(1, n_tensor)]
    core_peer = {"dp": z * 2 + 1 - core}
    z_peers = [{"dp": lax.rem(z + k, n_z) * 2 + core} for k in range(1, n_z)]
    barrier = pltpu.get_barrier_semaphore()
    for peer in (*x_peers, core_peer, *z_peers):
        pl.semaphore_signal(barrier, inc=1, device_id=peer, device_id_type=MESH)

    @pl.when(has_next)
    def _():
        pl.semaphore_signal(barrier, inc=1, device_id={"section": sec + 1}, device_id_type=MESH)

    @pl.when(has_prev)
    def _():
        pl.semaphore_signal(barrier, inc=1, device_id={"section": sec - 1}, device_id_type=MESH)

    def row_blocks(body):
        def step(i, carry):
            body(pl.ds(pl.multiple_of(i * ROW_BLOCK, ROW_BLOCK), ROW_BLOCK))
            return carry

        lax.fori_loop(0, rows // ROW_BLOCK, step, 0, unroll=True)

    def col_tiles(body):
        def step(i, carry):
            body(pl.ds(pl.multiple_of(i * TILE, TILE), TILE))
            return carry

        lax.fori_loop(0, cols // TILE, step, 0, unroll=2)

    gain_load.wait()
    gain_row = gain[...].astype(jnp.float32)

    def scale_down(r):
        down[r, :] = (down[r, :].astype(jnp.float32) * gain_row).astype(jnp.bfloat16)

    def squares_of(ref):
        def body(r):
            values = ref[r, :].astype(jnp.float32)
            values = values * values
            total = values[:, :128]
            for j in range(1, cols // 128):
                total = total + values[:, j * 128 : (j + 1) * 128]
            squares[r, :] = total

        row_blocks(body)
        return jnp.sum(squares[...], axis=1, keepdims=True)

    def place(which, part, total):
        part = part.astype(jnp.bfloat16)
        for r0, n in CHUNKS:
            at = 3 * r0 + which * n
            own[at : at + n, :units] = part[r0 : r0 + n]
            if total is not None:
                own[at : at + n, units:] = jnp.broadcast_to(total[r0 : r0 + n].astype(jnp.bfloat16), (n, 256 - units))

    loaded(down_load)
    row_blocks(scale_down)
    loaded(saved_load)
    place(1, contract(saved[...], down[...], (1, 1)), squares_of(saved))

    loaded(kept_load)
    lens_load.wait()

    def mask_rows(r):
        row = r.start + lax.broadcasted_iota(jnp.int32, (ROW_BLOCK, cols), 0)
        half = rows // 2
        second = row >= half
        position = jnp.where(second, row - half, row)
        limit = jnp.where(second, lens[1], lens[0])
        values = kept[r, :].astype(jnp.float32)
        kept[r, :] = jnp.where(position < limit, values, 0.0).astype(jnp.bfloat16)

    row_blocks(mask_rows)
    loaded(up_load)
    place(2, contract(kept[...], up[...], (1, 1)), None)
    loaded(fwd_load)
    place(0, contract(fwd[...], down[...], (1, 1)), squares_of(fwd))

    sections = (sec + n_section - 1) // n_section + (2 * n_section - 2 - sec) // n_section
    pl.semaphore_wait(barrier, n_tensor - 1 + 1 + n_z - 1 + sections)

    @pl.when(sec == 0)
    def _():
        next_f[...] = jnp.zeros_like(next_f)

    @pl.when(sec == n_section - 1)
    def _():
        next_g[...] = jnp.zeros_like(next_g)

    x_copies = []
    for c, (r0, n) in enumerate(CHUNKS):
        at = pl.ds(3 * r0, 3 * n)
        x_copies.append([
            remote(own.at[at], others.at[k, at], x_send.at[c, k], x_recv.at[c, k], x_peers[k])
            for k in range(n_tensor - 1)
        ])
        for copy in x_copies[-1]:
            copy.start()

    f_copies, b_copies = [], []
    for c, (r0, n) in enumerate(CHUNKS):
        for copy in x_copies[c]:
            copy.wait_recv()

        def summed(which):
            at = pl.ds(3 * r0 + which * n, n)
            total = own[at, :].astype(jnp.float32)
            for k in range(n_tensor - 1):
                total = total + others[k, at, :].astype(jnp.float32)
            return total

        r = pl.ds(r0, n)
        saved_total = summed(1)
        saved_scale = lax.rsqrt(saved_total[:, units : units + 1] / width + EPSILON)
        saved_rank = saved_total[:, :units] * saved_scale
        gate = jax.nn.sigmoid(saved_rank)
        sact_all[r, :] = (saved_rank * gate).astype(jnp.bfloat16)
        back = summed(2)[:, :units] * (gate * (1.0 + saved_rank * (1.0 - gate)))
        pull = saved_scale * saved_scale * (jnp.sum(back * saved_rank, axis=1, keepdims=True) / width)
        back = (back * saved_scale).astype(jnp.bfloat16)
        back_all[r, :] = back
        fwd_total = summed(0)
        fwd_scale = lax.rsqrt(fwd_total[:, units : units + 1] / width + EPSILON)
        act = jax.nn.silu(fwd_total[:, :units] * fwd_scale).astype(jnp.bfloat16)

        def back_tile(t):
            weighted = contract(back, down[:, t], (1, 0))
            values = kept[r, t].astype(jnp.float32) + weighted - saved[r, t].astype(jnp.float32) * pull
            back_out[r, t] = values.astype(jnp.bfloat16)

        col_tiles(back_tile)
        b_copies.append(remote(back_out.at[r], next_g.at[r], b_send.at[c], b_recv.at[c], {"section": sec - 1}))

        @pl.when(has_prev)
        def _():
            b_copies[c].start()

        def fwd_tile(t):
            raised = contract(act, up[:, t], (1, 0))
            fwd_out[r, t] = (fwd[r, t].astype(jnp.float32) + raised).astype(jnp.bfloat16)

        col_tiles(fwd_tile)
        f_copies.append(remote(fwd_out.at[r], next_f.at[r], f_send.at[c], f_recv.at[c], {"section": sec + 1}))

        @pl.when(has_next)
        def _():
            f_copies[c].start()

    def part_tile(t):
        share = units // n_dp
        down_part = (contract(back_all[...], saved[:, t], (0, 0)) * gain[:, t].astype(jnp.float32)).astype(jnp.bfloat16)
        up_part = contract(sact_all[...], kept[:, t], (0, 0)).astype(jnp.bfloat16)
        for i in range(n_dp):
            at = slice(i * share, (i + 1) * share)
            parts[i % 2, i // 2, 0, :, t] = down_part[at]
            parts[i % 2, i // 2, 1, :, t] = up_part[at]

    col_tiles(part_tile)
    order = [lax.rem(z + k, n_z) for k in (*range(1, n_z), 0)]
    c_copies = []
    for i, at in enumerate(order):
        c_copies.append(remote(parts.at[1 - core, at], from_core.at[i], c_send.at[i], c_recv.at[i], core_peer))
        c_copies[-1].start()
    z_copies = []
    for i, at in enumerate(order):
        c_copies[i].wait_recv()

        def add(t):
            for a in range(2):
                chip_sum[i, a, :, t] = (
                    parts[core, at, a, :, t].astype(jnp.float32) + from_core[i, a, :, t].astype(jnp.float32)
                ).astype(jnp.bfloat16)

        col_tiles(add)
        if i < n_z - 1:
            z_copies.append(remote(chip_sum.at[i], from_chip.at[i], z_send.at[i], z_recv.at[i], z_peers[i]))
            z_copies[-1].start()
    for copy in z_copies:
        copy.wait_recv()

    def finish(t):
        for a in range(2):
            total = chip_sum[n_z - 1, a, :, t].astype(jnp.float32)
            for i in range(n_z - 1):
                total = total + from_chip[i, a, :, t].astype(jnp.float32)
            (grad_down, grad_up)[a][:, t] = (total * (1.0 / n_dp)).astype(jnp.bfloat16)

    col_tiles(finish)

    for copies in x_copies:
        for copy in copies:
            copy.wait_send()
    for copy in (*c_copies, *z_copies):
        copy.wait_send()
    for c in range(len(CHUNKS)):
        @pl.when(has_prev)
        def _():
            b_copies[c].wait_send()
            f_copies[c].wait_recv()

        @pl.when(has_next)
        def _():
            f_copies[c].wait_send()
            b_copies[c].wait_recv()


def put_out(*refs):
    sources, targets, sem = refs[:4], refs[4:8], refs[8]
    copies = []
    for i in range(4):
        n = sources[i].shape[0] // PIECES
        for j in range(PIECES):
            at = pl.ds(j * n, n)
            copies.append(pltpu.make_async_copy(sources[i].at[at], targets[i].at[at], sem.at[i, j]))
            copies[-1].start()
    for copy in copies:
        copy.wait()


def solution(mesh):
    n_section, n_tensor, n_dp = (mesh.shape[a] for a in ("section", "tensor", "dp"))
    n_z = n_dp // 2

    def shards(forward_rows, saved_rows, output_grad, lengths, norm_gain, down_map, up_map):
        rows, cols = forward_rows.shape[2:]
        units = down_map.shape[1]
        share = units // n_dp
        n = len(CHUNKS)
        bf16 = jnp.bfloat16
        in_hbm = pl.BlockSpec(memory_space=pltpu.HBM)
        in_vmem = pl.BlockSpec(memory_space=pltpu.VMEM)
        dma = pltpu.SemaphoreType.DMA
        results = pl.pallas_call(
            functools.partial(kernel, n_section, n_tensor, n_dp),
            out_shape=(
                jax.ShapeDtypeStruct((rows, cols), bf16),
                jax.ShapeDtypeStruct((rows, cols), bf16),
                jax.ShapeDtypeStruct((share, cols), bf16),
                jax.ShapeDtypeStruct((share, cols), bf16),
            ),
            in_specs=[
                *[in_hbm] * 7,
            ],
            out_specs=(in_vmem,) * 4,
            scratch_shapes=[
                *[pltpu.VMEM((rows, cols), bf16)] * 3,
                *[pltpu.VMEM((units, cols), bf16)] * 2,
                pltpu.VMEM((rows, 128), jnp.float32),
                *[pltpu.VMEM((rows, cols), bf16)] * 2,
                pltpu.VMEM((3 * rows, 256), bf16),
                pltpu.VMEM((n_tensor - 1, 3 * rows, 256), bf16),
                *[pltpu.VMEM((rows, units), bf16)] * 2,
                pltpu.VMEM((2, n_z, 2, share, cols), bf16),
                pltpu.VMEM((n_z, 2, share, cols), bf16),
                pltpu.VMEM((n_z, 2, share, cols), bf16),
                pltpu.VMEM((n_z - 1, 2, share, cols), bf16),
                pltpu.SMEM((2,), jnp.int32),
                pltpu.VMEM((1, cols), bf16),
                dma((2,)),
                dma((5, PIECES)),
                *[dma((n, n_tensor - 1))] * 2,
                *[dma((n,))] * 4,
                *[dma((n_z,))] * 2,
                *[dma((n_z - 1,))] * 2,
            ],
            compiler_params=pltpu.CompilerParams(
                collective_id=0, has_side_effects=True, vmem_limit_bytes=48 * 1024 * 1024
            ),
        )(
            *(
                pltpu.with_memory_space_constraint(a, pltpu.HBM)
                for a in (
                    lengths[0, 0], norm_gain, forward_rows[0, 0], saved_rows[0, 0], output_grad[0, 0], down_map[0],
                    up_map[0],
                )
            )
        )
        got_f, got_g, grad_down, grad_up = pl.pallas_call(
            put_out,
            out_shape=tuple(jax.ShapeDtypeStruct(a.shape, a.dtype) for a in results),
            in_specs=[pl.BlockSpec(memory_space=pl.ANY)] * 4,
            out_specs=(in_hbm,) * 4,
            scratch_shapes=[dma((4, PIECES))],
        )(*(pltpu.with_memory_space_constraint(a, pltpu.VMEM) for a in results))
        return got_f[None, None], got_g[None, None], grad_down[None], grad_up[None]

    wide = P("section", "dp", None, "tensor")
    return jax.shard_map(
        shards,
        mesh=mesh,
        in_specs=(
            wide, wide, wide, P("section", "dp", None), P("section", "tensor"),
            P("section", None, "tensor"), P("section", None, "tensor"),
        ),
        out_specs=(wide, wide, P("section", "dp", "tensor"), P("section", "dp", "tensor")),
        check_vma=False,
    )
```

```python
import functools

import jax
import jax.numpy as jnp
from jax import lax
from jax.experimental import pallas as pl
from jax.experimental.pallas import tpu as pltpu
from jax.sharding import PartitionSpec as P

EPSILON = 1e-05
MESH = pl.DeviceIdType.MESH
CHUNKS = ((0, 16), (16, 32), (48, 64), (112, 80))
TILE = 256
ROW_BLOCK = 16
PIECES = 4
EARLY_EVERY = 4
HEAD = CHUNKS[0][1]


def remote(src, dst, send_sem, recv_sem, target):
    return pltpu.make_async_remote_copy(
        src_ref=src, dst_ref=dst, send_sem=send_sem, recv_sem=recv_sem, device_id=target, device_id_type=MESH
    )


def contract(left, right, dims):
    return lax.dot_general(left, right, ((dims[:1], dims[1:]), ((), ())), preferred_element_type=jnp.float32)


def kernel(
    n_section, n_tensor, n_dp,
    lens_hbm, gain_hbm, f_hbm, s_hbm, g_hbm, d_hbm, u_hbm,
    next_f, next_g, grad_down, grad_up,
    fwd, saved, kept, down, up, squares, fwd_out, back_out, own, others, sact_all, back_all,
    parts, from_core, chip_sum, from_chip,
    lens, gain, near, far, small_sem, load_sem, x_send, x_recv, f_send, f_recv, b_send, b_recv, c_send, c_recv, z_send, z_recv,
):
    rows, cols = fwd.shape
    units = down.shape[0]
    width = cols * n_tensor
    sec, ten, dp = lax.axis_index("section"), lax.axis_index("tensor"), lax.axis_index("dp")
    n_z = n_dp // 2
    z, core = dp // 2, dp % 2
    early = jnp.logical_and(lax.rem(sec, EARLY_EVERY) == 0, sec > 0)
    has_next, has_prev = sec < n_section - 1, sec > 0

    lens_load = pltpu.make_async_copy(lens_hbm, lens, small_sem.at[0])
    gain_load = pltpu.make_async_copy(gain_hbm, gain, small_sem.at[1])

    def pieces_of(i, src, dst, bounds):
        return [
            pltpu.make_async_copy(src.at[pl.ds(lo, hi - lo)], dst.at[pl.ds(lo, hi - lo)], load_sem.at[i, j])
            for j, (lo, hi) in enumerate(zip(bounds, bounds[1:]))
        ]

    quarters = tuple(range(0, units + 1, units // PIECES))
    row_bounds = (0, HEAD, rows // 2, rows)
    down_load = pieces_of(0, d_hbm, down, quarters)
    up_load = pieces_of(1, u_hbm, up, quarters)
    saved_load = pieces_of(2, s_hbm, saved, row_bounds)
    fwd_load = pieces_of(3, f_hbm, fwd, row_bounds)
    kept_load = pieces_of(4, g_hbm, kept, row_bounds)
    for copy in (
        gain_load, *down_load, saved_load[0], fwd_load[0], lens_load, kept_load[0], *up_load,
        *saved_load[1:], *fwd_load[1:], *kept_load[1:],
    ):
        copy.start()

    def loaded(pieces):
        for piece in pieces:
            piece.wait()

    x_peers = [{"tensor": lax.rem(ten + k, n_tensor)} for k in range(1, n_tensor)]
    core_peer = {"dp": z * 2 + 1 - core}
    z_peers = [{"dp": lax.rem(z + k, n_z) * 2 + core} for k in range(1, n_z)]
    barrier = pltpu.get_barrier_semaphore()

    def enter(peer):
        pl.semaphore_signal(barrier, inc=1, device_id=peer, device_id_type=MESH)

    for k in range(1, n_tensor):
        enter({"tensor": lax.rem(ten + k, n_tensor), "dp": z * 2})
    for k in range(1, n_z):
        enter({"dp": lax.rem(z + k, n_z) * 2})

    @pl.when(core == 1)
    def _():
        enter({"dp": z * 2})

    @pl.when(has_next)
    def _():
        enter({"section": sec + 1, "dp": z * 2 + 1})

    @pl.when(has_prev)
    def _():
        enter({"section": sec - 1, "dp": z * 2 + 1})

    def meet_near():
        @pl.when(core == 0)
        def _():
            pl.semaphore_wait(barrier, 2 * (n_tensor - 1) + 2 * (n_z - 1) + 1)
            pl.semaphore_signal(near, inc=1, device_id=core_peer, device_id_type=MESH)

        @pl.when(core == 1)
        def _():
            pl.semaphore_wait(near, 1)

    def meet_sections():
        @pl.when(core == 1)
        def _():
            sections = (sec + n_section - 1) // n_section + (2 * n_section - 2 - sec) // n_section
            pl.semaphore_wait(barrier, 2 * sections)
            pl.semaphore_signal(far, inc=1, device_id=core_peer, device_id_type=MESH)

        @pl.when(core == 0)
        def _():
            pl.semaphore_wait(far, 1)

    def row_blocks(body, lo, hi):
        def step(i, carry):
            body(pl.ds(pl.multiple_of(i * ROW_BLOCK, ROW_BLOCK), ROW_BLOCK))
            return carry

        lax.fori_loop(lo // ROW_BLOCK, hi // ROW_BLOCK, step, 0, unroll=True)

    def col_tiles(body, unroll=2):
        def step(i, carry):
            body(pl.ds(pl.multiple_of(i * TILE, TILE), TILE))
            return carry

        lax.fori_loop(0, cols // TILE, step, 0, unroll=unroll)

    def squares_of(ref, lo, hi):
        def body(r):
            values = ref[r, :].astype(jnp.float32)
            values = values * values
            total = values[:, :128]
            for j in range(1, cols // 128):
                total = total + values[:, j * 128 : (j + 1) * 128]
            squares[r, :] = total

        row_blocks(body, lo, hi)
        return jnp.sum(squares[lo:hi, :], axis=1, keepdims=True)

    def mask_rows(r):
        row = r.start + lax.broadcasted_iota(jnp.int32, (ROW_BLOCK, cols), 0)
        half = rows // 2
        second = row >= half
        position = jnp.where(second, row - half, row)
        limit = jnp.where(second, lens[1], lens[0])
        values = kept[r, :].astype(jnp.float32)
        kept[r, :] = jnp.where(position < limit, values, 0.0).astype(jnp.bfloat16)

    def place(which, part, total, chunks):
        base = chunks[0][0]
        part = part.astype(jnp.bfloat16)
        for r0, n in chunks:
            at = 3 * r0 + which * n
            own[at : at + n, :units] = part[r0 - base : r0 - base + n]
            if total is not None:
                spread = jnp.broadcast_to(total[r0 - base : r0 - base + n].astype(jnp.bfloat16), (n, 256 - units))
                own[at : at + n, units:] = spread

    x_copies = []
    for c, (r0, n) in enumerate(CHUNKS):
        at = pl.ds(3 * r0, 3 * n)
        x_copies.append([
            remote(own.at[at], others.at[k, at], x_send.at[c, k], x_recv.at[c, k], x_peers[k])
            for k in range(n_tensor - 1)
        ])

    gain_load.wait()
    gain_row = gain[...].astype(jnp.float32)

    def scale_down(r):
        down[r, :] = (down[r, :].astype(jnp.float32) * gain_row).astype(jnp.bfloat16)

    head, rest = CHUNKS[:1], CHUNKS[1:]
    loaded(down_load)
    row_blocks(scale_down, 0, units)
    loaded((saved_load[0], fwd_load[0]))
    both = contract(jnp.concatenate([saved[:HEAD, :], fwd[:HEAD, :]], axis=0), down[...], (1, 1))
    place(1, both[:HEAD], squares_of(saved, 0, HEAD), head)
    place(0, both[HEAD:], squares_of(fwd, 0, HEAD), head)
    loaded((kept_load[0], lens_load))
    row_blocks(mask_rows, 0, HEAD)
    loaded(up_load)
    place(2, contract(kept[:HEAD, :], up[...], (1, 1)), None, head)
    with jax.named_scope("near"):
        meet_near()
    for copy in x_copies[0]:
        copy.start()

    loaded(saved_load[1:])
    place(1, contract(saved[HEAD:, :], down[...], (1, 1)), squares_of(saved, HEAD, rows), rest)
    loaded(fwd_load[1:])
    place(0, contract(fwd[HEAD:, :], down[...], (1, 1)), squares_of(fwd, HEAD, rows), rest)
    loaded(kept_load[1:])
    row_blocks(mask_rows, HEAD, rows)
    place(2, contract(kept[HEAD:, :], up[...], (1, 1)), None, rest)
    for copies in x_copies[1:]:
        for copy in copies:
            copy.start()

    @pl.when(sec == 0)
    def _():
        next_f[...] = jnp.zeros_like(next_f)

    @pl.when(sec == n_section - 1)
    def _():
        next_g[...] = jnp.zeros_like(next_g)

    f_copies, b_copies = [], []

    def send_rows(c):
        @pl.when(has_prev)
        def _():
            b_copies[c].start()

        @pl.when(has_next)
        def _():
            f_copies[c].start()

    for c, (r0, n) in enumerate(CHUNKS):
        with jax.named_scope(f"x{c}"):
            for copy in x_copies[c]:
                copy.wait_recv()

        def summed(which):
            at = pl.ds(3 * r0 + which * n, n)
            total = own[at, :].astype(jnp.float32)
            for k in range(n_tensor - 1):
                total = total + others[k, at, :].astype(jnp.float32)
            return total

        r = pl.ds(r0, n)
        saved_total = summed(1)
        saved_scale = lax.rsqrt(saved_total[:, units : units + 1] / width + EPSILON)
        saved_rank = saved_total[:, :units] * saved_scale
        gate = jax.nn.sigmoid(saved_rank)
        sact_all[r, :] = (saved_rank * gate).astype(jnp.bfloat16)
        back = summed(2)[:, :units] * (gate * (1.0 + saved_rank * (1.0 - gate)))
        pull = saved_scale * saved_scale * (jnp.sum(back * saved_rank, axis=1, keepdims=True) / width)
        back = (back * saved_scale).astype(jnp.bfloat16)
        back_all[r, :] = back
        fwd_total = summed(0)
        fwd_scale = lax.rsqrt(fwd_total[:, units : units + 1] / width + EPSILON)
        act = jax.nn.silu(fwd_total[:, :units] * fwd_scale).astype(jnp.bfloat16)

        def back_tile(t):
            weighted = contract(back, down[:, t], (1, 0))
            values = kept[r, t].astype(jnp.float32) + weighted - saved[r, t].astype(jnp.float32) * pull
            back_out[r, t] = values.astype(jnp.bfloat16)

        col_tiles(back_tile, 2 if c else True)
        b_copies.append(remote(back_out.at[r], next_g.at[r], b_send.at[c], b_recv.at[c], {"section": sec - 1}))

        def fwd_tile(t):
            raised = contract(act, up[:, t], (1, 0))
            fwd_out[r, t] = (fwd[r, t].astype(jnp.float32) + raised).astype(jnp.bfloat16)

        col_tiles(fwd_tile, 2 if c else True)
        f_copies.append(remote(fwd_out.at[r], next_f.at[r], f_send.at[c], f_recv.at[c], {"section": sec + 1}))
        if c == 0:
            with jax.named_scope("sections"):
                meet_sections()
        if c < len(CHUNKS) - 1:
            send_rows(c)
        else:
            @pl.when(jnp.logical_not(early))
            def _():
                send_rows(c)

    def part_tile(t):
        share = units // n_dp
        down_part = (contract(back_all[...], saved[:, t], (0, 0)) * gain[:, t].astype(jnp.float32)).astype(jnp.bfloat16)
        up_part = contract(sact_all[...], kept[:, t], (0, 0)).astype(jnp.bfloat16)
        for i in range(n_dp):
            at = slice(i * share, (i + 1) * share)
            parts[i % 2, i // 2, 0, :, t] = down_part[at]
            parts[i % 2, i // 2, 1, :, t] = up_part[at]

    with jax.named_scope("parts"):
        col_tiles(part_tile)
    order = [lax.rem(z + k, n_z) for k in (*range(1, n_z), 0)]
    c_copies = []
    for i, at in enumerate(order):
        c_copies.append(remote(parts.at[1 - core, at], from_core.at[i], c_send.at[i], c_recv.at[i], core_peer))
        c_copies[-1].start()
    z_copies = []
    for i, at in enumerate(order):
        with jax.named_scope(f"c{i}"):
            c_copies[i].wait_recv()

        def add(t):
            for a in range(2):
                chip_sum[i, a, :, t] = (
                    parts[core, at, a, :, t].astype(jnp.float32) + from_core[i, a, :, t].astype(jnp.float32)
                ).astype(jnp.bfloat16)

        col_tiles(add)
        if i < n_z - 1:
            z_copies.append(remote(chip_sum.at[i], from_chip.at[i], z_send.at[i], z_recv.at[i], z_peers[i]))
            z_copies[-1].start()

    @pl.when(early)
    def _():
        send_rows(len(CHUNKS) - 1)

    with jax.named_scope("z"):
        for copy in z_copies:
            copy.wait_recv()

    def finish(t):
        for a in range(2):
            total = chip_sum[n_z - 1, a, :, t].astype(jnp.float32)
            for i in range(n_z - 1):
                total = total + from_chip[i, a, :, t].astype(jnp.float32)
            (grad_down, grad_up)[a][:, t] = (total * (1.0 / n_dp)).astype(jnp.bfloat16)

    col_tiles(finish)

    for copies in x_copies:
        for copy in copies:
            copy.wait_send()
    for c in range(len(CHUNKS)):
        with jax.named_scope(f"f{c}"):
            @pl.when(has_prev)
            def _():
                f_copies[c].wait_recv()

        with jax.named_scope(f"b{c}"):
            @pl.when(has_next)
            def _():
                b_copies[c].wait_recv()

    with jax.named_scope("sent"):
        for copy in (*c_copies, *z_copies):
            copy.wait_send()
        for c in range(len(CHUNKS)):
            @pl.when(has_prev)
            def _():
                b_copies[c].wait_send()

            @pl.when(has_next)
            def _():
                f_copies[c].wait_send()


def put_out(*refs):
    sources, targets, sem = refs[:4], refs[4:8], refs[8]
    copies = []
    for i in range(4):
        n = sources[i].shape[0] // PIECES
        for j in range(PIECES):
            at = pl.ds(j * n, n)
            copies.append(pltpu.make_async_copy(sources[i].at[at], targets[i].at[at], sem.at[i, j]))
            copies[-1].start()
    for copy in copies:
        copy.wait()


def solution(mesh):
    n_section, n_tensor, n_dp = (mesh.shape[a] for a in ("section", "tensor", "dp"))
    n_z = n_dp // 2

    def shards(forward_rows, saved_rows, output_grad, lengths, norm_gain, down_map, up_map):
        rows, cols = forward_rows.shape[2:]
        units = down_map.shape[1]
        share = units // n_dp
        n = len(CHUNKS)
        bf16 = jnp.bfloat16
        in_hbm = pl.BlockSpec(memory_space=pltpu.HBM)
        in_vmem = pl.BlockSpec(memory_space=pltpu.VMEM)
        dma = pltpu.SemaphoreType.DMA
        results = pl.pallas_call(
            functools.partial(kernel, n_section, n_tensor, n_dp),
            out_shape=(
                jax.ShapeDtypeStruct((rows, cols), bf16),
                jax.ShapeDtypeStruct((rows, cols), bf16),
                jax.ShapeDtypeStruct((share, cols), bf16),
                jax.ShapeDtypeStruct((share, cols), bf16),
            ),
            in_specs=[
                *[in_hbm] * 7,
            ],
            out_specs=(in_vmem,) * 4,
            scratch_shapes=[
                *[pltpu.VMEM((rows, cols), bf16)] * 3,
                *[pltpu.VMEM((units, cols), bf16)] * 2,
                pltpu.VMEM((rows, 128), jnp.float32),
                *[pltpu.VMEM((rows, cols), bf16)] * 2,
                pltpu.VMEM((3 * rows, 256), bf16),
                pltpu.VMEM((n_tensor - 1, 3 * rows, 256), bf16),
                *[pltpu.VMEM((rows, units), bf16)] * 2,
                pltpu.VMEM((2, n_z, 2, share, cols), bf16),
                pltpu.VMEM((n_z, 2, share, cols), bf16),
                pltpu.VMEM((n_z, 2, share, cols), bf16),
                pltpu.VMEM((n_z - 1, 2, share, cols), bf16),
                pltpu.SMEM((2,), jnp.int32),
                pltpu.VMEM((1, cols), bf16),
                *[pltpu.SemaphoreType.REGULAR] * 2,
                dma((2,)),
                dma((5, PIECES)),
                *[dma((n, n_tensor - 1))] * 2,
                *[dma((n,))] * 4,
                *[dma((n_z,))] * 2,
                *[dma((n_z - 1,))] * 2,
            ],
            compiler_params=pltpu.CompilerParams(
                collective_id=0, has_side_effects=True, vmem_limit_bytes=48 * 1024 * 1024
            ),
        )(
            *(
                pltpu.with_memory_space_constraint(a, pltpu.HBM)
                for a in (
                    lengths[0, 0], norm_gain, forward_rows[0, 0], saved_rows[0, 0], output_grad[0, 0], down_map[0],
                    up_map[0],
                )
            )
        )
        got_f, got_g, grad_down, grad_up = pl.pallas_call(
            put_out,
            out_shape=tuple(jax.ShapeDtypeStruct(a.shape, a.dtype) for a in results),
            in_specs=[pl.BlockSpec(memory_space=pl.ANY)] * 4,
            out_specs=(in_hbm,) * 4,
            scratch_shapes=[dma((4, PIECES))],
        )(*(pltpu.with_memory_space_constraint(a, pltpu.VMEM) for a in results))
        return got_f[None, None], got_g[None, None], grad_down[None], grad_up[None]

    wide = P("section", "dp", None, "tensor")
    return jax.shard_map(
        shards,
        mesh=mesh,
        in_specs=(
            wide, wide, wide, P("section", "dp", None), P("section", "tensor"),
            P("section", None, "tensor"), P("section", None, "tensor"),
        ),
        out_specs=(wide, wide, P("section", "dp", "tensor"), P("section", "dp", "tensor")),
        check_vma=False,
    )
```

```python
import functools

import jax
import jax.numpy as jnp
from jax import lax
from jax.experimental import pallas as pl
from jax.experimental.pallas import tpu as pltpu
from jax.sharding import PartitionSpec as P

EPSILON = 1e-05
MESH = pl.DeviceIdType.MESH
CHUNKS = ((0, 16), (16, 32), (48, 64), (112, 80))
TILE = 256
ROW_BLOCK = 16
PIECES = 4
EARLY_EVERY = 4
HEAD = CHUNKS[0][1]


def remote(src, dst, send_sem, recv_sem, target):
    return pltpu.make_async_remote_copy(
        src_ref=src, dst_ref=dst, send_sem=send_sem, recv_sem=recv_sem, device_id=target, device_id_type=MESH
    )


def contract(left, right, dims):
    return lax.dot_general(left, right, ((dims[:1], dims[1:]), ((), ())), preferred_element_type=jnp.float32)


def kernel(
    n_section, n_tensor, n_dp,
    lens_hbm, gain_hbm, f_hbm, s_hbm, g_hbm, d_hbm, u_hbm,
    next_f, next_g, grad_down, grad_up,
    fwd, saved, kept, down, up, squares, fwd_out, back_out, own, others, sact_all, back_all,
    parts, from_core, chip_sum, from_chip,
    lens, gain, near, far_next, far_prev, mate, small_sem, load_sem, x_send, x_recv, f_send, f_recv, b_send, b_recv, c_send, c_recv, z_send, z_recv,
):
    rows, cols = fwd.shape
    units = down.shape[0]
    width = cols * n_tensor
    sec, ten, dp = lax.axis_index("section"), lax.axis_index("tensor"), lax.axis_index("dp")
    n_z = n_dp // 2
    z, core = dp // 2, dp % 2
    early = lax.rem(sec, EARLY_EVERY) == 0
    dp_first = jnp.logical_and(early, sec > 0)
    has_next, has_prev = sec < n_section - 1, sec > 0

    lens_load = pltpu.make_async_copy(lens_hbm, lens, small_sem.at[0])
    gain_load = pltpu.make_async_copy(gain_hbm, gain, small_sem.at[1])

    def pieces_of(i, src, dst, bounds):
        return [
            pltpu.make_async_copy(src.at[pl.ds(lo, hi - lo)], dst.at[pl.ds(lo, hi - lo)], load_sem.at[i, j])
            for j, (lo, hi) in enumerate(zip(bounds, bounds[1:]))
        ]

    quarters = tuple(range(0, units + 1, units // PIECES))
    row_bounds = (0, HEAD, rows // 2, rows)
    down_load = pieces_of(0, d_hbm, down, quarters)
    up_load = pieces_of(1, u_hbm, up, quarters)
    saved_load = pieces_of(2, s_hbm, saved, row_bounds)
    fwd_load = pieces_of(3, f_hbm, fwd, row_bounds)
    kept_load = pieces_of(4, g_hbm, kept, row_bounds)
    for copy in (
        gain_load, *down_load, saved_load[0], fwd_load[0], lens_load, kept_load[0], *up_load,
        *saved_load[1:], *fwd_load[1:], *kept_load[1:],
    ):
        copy.start()

    def loaded(pieces):
        for piece in pieces:
            piece.wait()

    x_peers = [{"tensor": lax.rem(ten + k, n_tensor)} for k in range(1, n_tensor)]
    core_peer = {"dp": z * 2 + 1 - core}
    z_peers = [{"dp": lax.rem(z + k, n_z) * 2 + core} for k in range(1, n_z)]
    barrier = pltpu.get_barrier_semaphore()
    odd = lax.rem(ten, 2)
    pair = ten - odd

    def signal(sem, peer):
        pl.semaphore_signal(sem, inc=1, device_id=peer, device_id_type=MESH)

    def of_pair(place, which):
        return {"tensor": pair + place, "dp": z * 2 + which}

    even0, odd0, even1, odd1 = of_pair(0, 0), of_pair(1, 0), of_pair(0, 1), of_pair(1, 1)
    is_even0, is_odd0, is_even1, is_odd1 = (
        jnp.logical_and(odd == place, core == which) for which in range(2) for place in range(2)
    )

    for k in range(0, n_tensor, 2):
        ear = {"tensor": lax.rem(pair + k, n_tensor) + core, "dp": z * 2}
        if k:
            signal(barrier, ear)
        else:
            @pl.when(jnp.logical_not(is_even0))
            def _():
                signal(barrier, ear)

    @pl.when(has_prev)
    def _():
        signal(barrier, {"section": sec - 1, "tensor": pair, "dp": z * 2 + 1})

    @pl.when(has_next)
    def _():
        signal(barrier, {"section": sec + 1, "tensor": pair + 1, "dp": z * 2 + 1})

    for k in range(1, n_z):
        signal(barrier, {"tensor": pair + 1, "dp": lax.rem(z + k, n_z) * 2 + 1})

    def tell_near():
        @pl.when(is_even0)
        def _():
            pl.semaphore_wait(barrier, n_tensor - 1)
            signal(near, odd0)

        @pl.when(is_odd0)
        def _():
            pl.semaphore_wait(barrier, n_tensor)
            signal(near, even1)
            signal(near, odd1)

    def meet_near():
        @pl.when(jnp.logical_not(is_even0))
        def _():
            pl.semaphore_wait(near, 1)

    def tell_next():
        @pl.when(is_even1)
        def _():
            @pl.when(has_next)
            def _():
                pl.semaphore_wait(barrier, 4)

            signal(far_next, odd0)
            signal(far_next, odd1)

    def meet_next():
        @pl.when(jnp.logical_not(is_even1))
        def _():
            pl.semaphore_wait(far_next, 1)

        @pl.when(is_odd0)
        def _():
            signal(far_next, even0)

        @pl.when(is_even0)
        def _():
            signal(mate, even1)

    def tell_prev():
        @pl.when(is_odd1)
        def _():
            pl.semaphore_wait(barrier, 4 * ((sec + n_section - 1) // n_section) + 4 * (n_z - 1))
            signal(far_prev, odd0)
            signal(far_prev, even1)

    def meet_prev():
        @pl.when(jnp.logical_not(is_odd1))
        def _():
            pl.semaphore_wait(far_prev, 1)

        @pl.when(is_odd0)
        def _():
            signal(far_prev, even0)

    def meet_mate():
        @pl.when(is_even1)
        def _():
            pl.semaphore_wait(mate, 1)

    def row_blocks(body, lo, hi):
        def step(i, carry):
            body(pl.ds(pl.multiple_of(i * ROW_BLOCK, ROW_BLOCK), ROW_BLOCK))
            return carry

        lax.fori_loop(lo // ROW_BLOCK, hi // ROW_BLOCK, step, 0, unroll=True)

    def col_tiles(body, unroll=2):
        def step(i, carry):
            body(pl.ds(pl.multiple_of(i * TILE, TILE), TILE))
            return carry

        lax.fori_loop(0, cols // TILE, step, 0, unroll=unroll)

    def squares_of(ref, lo, hi):
        def body(r):
            values = ref[r, :].astype(jnp.float32)
            values = values * values
            total = values[:, :128]
            for j in range(1, cols // 128):
                total = total + values[:, j * 128 : (j + 1) * 128]
            squares[r, :] = total

        row_blocks(body, lo, hi)
        return jnp.sum(squares[lo:hi, :], axis=1, keepdims=True)

    def mask_rows(r):
        row = r.start + lax.broadcasted_iota(jnp.int32, (ROW_BLOCK, cols), 0)
        half = rows // 2
        second = row >= half
        position = jnp.where(second, row - half, row)
        limit = jnp.where(second, lens[1], lens[0])
        values = kept[r, :].astype(jnp.float32)
        kept[r, :] = jnp.where(position < limit, values, 0.0).astype(jnp.bfloat16)

    def place(which, part, total, chunks):
        base = chunks[0][0]
        part = part.astype(jnp.bfloat16)
        for r0, n in chunks:
            at = 3 * r0 + which * n
            own[at : at + n, :units] = part[r0 - base : r0 - base + n]
            if total is not None:
                spread = jnp.broadcast_to(total[r0 - base : r0 - base + n].astype(jnp.bfloat16), (n, 256 - units))
                own[at : at + n, units:] = spread

    x_copies = []
    for c, (r0, n) in enumerate(CHUNKS):
        at = pl.ds(3 * r0, 3 * n)
        x_copies.append([
            remote(own.at[at], others.at[k, at], x_send.at[c, k], x_recv.at[c, k], x_peers[k])
            for k in range(n_tensor - 1)
        ])

    gain_load.wait()
    gain_row = gain[...].astype(jnp.float32)

    def scale_down(r):
        down[r, :] = (down[r, :].astype(jnp.float32) * gain_row).astype(jnp.bfloat16)

    head, rest = CHUNKS[:1], CHUNKS[1:]
    with jax.named_scope("ldd"):
        loaded(down_load)
    row_blocks(scale_down, 0, units)
    with jax.named_scope("ldh"):
        loaded((saved_load[0], fwd_load[0]))
    both = contract(jnp.concatenate([saved[:HEAD, :], fwd[:HEAD, :]], axis=0), down[...], (1, 1))
    place(1, both[:HEAD], squares_of(saved, 0, HEAD), head)
    place(0, both[HEAD:], squares_of(fwd, 0, HEAD), head)
    tell_near()
    loaded((kept_load[0], lens_load))
    row_blocks(mask_rows, 0, HEAD)
    with jax.named_scope("ldu"):
        loaded(up_load)
    place(2, contract(kept[:HEAD, :], up[...], (1, 1)), None, head)
    with jax.named_scope("near"):
        meet_near()
    for copy in x_copies[0]:
        copy.start()

    loaded(saved_load[1:])
    place(1, contract(saved[HEAD:, :], down[...], (1, 1)), squares_of(saved, HEAD, rows), rest)
    loaded(fwd_load[1:])
    place(0, contract(fwd[HEAD:, :], down[...], (1, 1)), squares_of(fwd, HEAD, rows), rest)
    loaded(kept_load[1:])
    row_blocks(mask_rows, HEAD, rows)
    place(2, contract(kept[HEAD:, :], up[...], (1, 1)), None, rest)
    for copies in x_copies[1:]:
        for copy in copies:
            copy.start()

    with jax.named_scope("tell"):
        tell_next()

        @pl.when(jnp.logical_not(early))
        def _():
            tell_prev()

    @pl.when(sec == 0)
    def _():
        next_f[...] = jnp.zeros_like(next_f)

    @pl.when(sec == n_section - 1)
    def _():
        next_g[...] = jnp.zeros_like(next_g)

    f_copies, b_copies = [], []

    def send_back(c):
        @pl.when(has_prev)
        def _():
            b_copies[c].start()

    def send_fwd(c):
        @pl.when(has_next)
        def _():
            f_copies[c].start()

    for c, (r0, n) in enumerate(CHUNKS):
        with jax.named_scope(f"x{c}"):
            for copy in x_copies[c]:
                copy.wait_recv()

        def summed(which):
            at = pl.ds(3 * r0 + which * n, n)
            total = own[at, :].astype(jnp.float32)
            for k in range(n_tensor - 1):
                total = total + others[k, at, :].astype(jnp.float32)
            return total

        r = pl.ds(r0, n)
        saved_total = summed(1)
        saved_scale = lax.rsqrt(saved_total[:, units : units + 1] / width + EPSILON)
        saved_rank = saved_total[:, :units] * saved_scale
        gate = jax.nn.sigmoid(saved_rank)
        sact_all[r, :] = (saved_rank * gate).astype(jnp.bfloat16)
        back = summed(2)[:, :units] * (gate * (1.0 + saved_rank * (1.0 - gate)))
        pull = saved_scale * saved_scale * (jnp.sum(back * saved_rank, axis=1, keepdims=True) / width)
        back = (back * saved_scale).astype(jnp.bfloat16)
        back_all[r, :] = back
        fwd_total = summed(0)
        fwd_scale = lax.rsqrt(fwd_total[:, units : units + 1] / width + EPSILON)
        act = jax.nn.silu(fwd_total[:, :units] * fwd_scale).astype(jnp.bfloat16)

        def back_tile(t):
            weighted = contract(back, down[:, t], (1, 0))
            values = kept[r, t].astype(jnp.float32) + weighted - saved[r, t].astype(jnp.float32) * pull
            back_out[r, t] = values.astype(jnp.bfloat16)

        col_tiles(back_tile, 2 if c else True)
        b_copies.append(remote(back_out.at[r], next_g.at[r], b_send.at[c], b_recv.at[c], {"section": sec - 1}))

        if c == 0:
            @pl.when(jnp.logical_not(early))
            def _():
                with jax.named_scope("prev"):
                    meet_prev()
                send_back(c)
        elif c < len(CHUNKS) - 1:
            @pl.when(jnp.logical_not(early))
            def _():
                send_back(c)

        def fwd_tile(t):
            raised = contract(act, up[:, t], (1, 0))
            fwd_out[r, t] = (fwd[r, t].astype(jnp.float32) + raised).astype(jnp.bfloat16)

        col_tiles(fwd_tile, 2 if c else True)
        f_copies.append(remote(fwd_out.at[r], next_f.at[r], f_send.at[c], f_recv.at[c], {"section": sec + 1}))
        if c == 0:
            with jax.named_scope("next"):
                meet_next()
        if c < len(CHUNKS) - 1:
            send_fwd(c)
        if c == 1:
            @pl.when(early)
            def _():
                with jax.named_scope("prevlate"):
                    tell_prev()
                    meet_prev()
                send_back(0)
                send_back(1)
        if c == 2:
            @pl.when(early)
            def _():
                send_back(c)
        if c == len(CHUNKS) - 1:
            @pl.when(jnp.logical_not(dp_first))
            def _():
                send_back(c)
                send_fwd(c)

    def part_tile(t):
        share = units // n_dp
        down_part = (contract(back_all[...], saved[:, t], (0, 0)) * gain[:, t].astype(jnp.float32)).astype(jnp.bfloat16)
        up_part = contract(sact_all[...], kept[:, t], (0, 0)).astype(jnp.bfloat16)
        for i in range(n_dp):
            at = slice(i * share, (i + 1) * share)
            parts[i % 2, i // 2, 0, :, t] = down_part[at]
            parts[i % 2, i // 2, 1, :, t] = up_part[at]

    with jax.named_scope("parts"):
        col_tiles(part_tile)
    meet_mate()
    order = [lax.rem(z + k, n_z) for k in (*range(1, n_z), 0)]
    c_copies = []
    for i, at in enumerate(order):
        c_copies.append(remote(parts.at[1 - core, at], from_core.at[i], c_send.at[i], c_recv.at[i], core_peer))
        c_copies[-1].start()
    z_copies = []
    for i, at in enumerate(order):
        with jax.named_scope(f"c{i}"):
            c_copies[i].wait_recv()

        def add(t):
            for a in range(2):
                chip_sum[i, a, :, t] = (
                    parts[core, at, a, :, t].astype(jnp.float32) + from_core[i, a, :, t].astype(jnp.float32)
                ).astype(jnp.bfloat16)

        col_tiles(add)
        if i < n_z - 1:
            z_copies.append(remote(chip_sum.at[i], from_chip.at[i], z_send.at[i], z_recv.at[i], z_peers[i]))
            z_copies[-1].start()

    @pl.when(dp_first)
    def _():
        send_back(len(CHUNKS) - 1)
        send_fwd(len(CHUNKS) - 1)

    with jax.named_scope("z"):
        for copy in z_copies:
            copy.wait_recv()

    def finish(t):
        for a in range(2):
            total = chip_sum[n_z - 1, a, :, t].astype(jnp.float32)
            for i in range(n_z - 1):
                total = total + from_chip[i, a, :, t].astype(jnp.float32)
            (grad_down, grad_up)[a][:, t] = (total * (1.0 / n_dp)).astype(jnp.bfloat16)

    col_tiles(finish)

    for copies in x_copies:
        for copy in copies:
            copy.wait_send()
    for c in range(len(CHUNKS)):
        with jax.named_scope(f"f{c}"):
            @pl.when(has_prev)
            def _():
                f_copies[c].wait_recv()

        with jax.named_scope(f"b{c}"):
            @pl.when(has_next)
            def _():
                b_copies[c].wait_recv()

    with jax.named_scope("sent"):
        for copy in (*c_copies, *z_copies):
            copy.wait_send()
        for c in range(len(CHUNKS)):
            @pl.when(has_prev)
            def _():
                b_copies[c].wait_send()

            @pl.when(has_next)
            def _():
                f_copies[c].wait_send()


def put_out(*refs):
    sources, targets, sem = refs[:4], refs[4:8], refs[8]
    copies = []
    for i in range(4):
        n = sources[i].shape[0] // PIECES
        for j in range(PIECES):
            at = pl.ds(j * n, n)
            copies.append(pltpu.make_async_copy(sources[i].at[at], targets[i].at[at], sem.at[i, j]))
            copies[-1].start()
    for copy in copies:
        copy.wait()


def solution(mesh):
    n_section, n_tensor, n_dp = (mesh.shape[a] for a in ("section", "tensor", "dp"))
    n_z = n_dp // 2

    def shards(forward_rows, saved_rows, output_grad, lengths, norm_gain, down_map, up_map):
        rows, cols = forward_rows.shape[2:]
        units = down_map.shape[1]
        share = units // n_dp
        n = len(CHUNKS)
        bf16 = jnp.bfloat16
        in_hbm = pl.BlockSpec(memory_space=pltpu.HBM)
        in_vmem = pl.BlockSpec(memory_space=pltpu.VMEM)
        dma = pltpu.SemaphoreType.DMA
        results = pl.pallas_call(
            functools.partial(kernel, n_section, n_tensor, n_dp),
            out_shape=(
                jax.ShapeDtypeStruct((rows, cols), bf16),
                jax.ShapeDtypeStruct((rows, cols), bf16),
                jax.ShapeDtypeStruct((share, cols), bf16),
                jax.ShapeDtypeStruct((share, cols), bf16),
            ),
            in_specs=[
                *[in_hbm] * 7,
            ],
            out_specs=(in_vmem,) * 4,
            scratch_shapes=[
                *[pltpu.VMEM((rows, cols), bf16)] * 3,
                *[pltpu.VMEM((units, cols), bf16)] * 2,
                pltpu.VMEM((rows, 128), jnp.float32),
                *[pltpu.VMEM((rows, cols), bf16)] * 2,
                pltpu.VMEM((3 * rows, 256), bf16),
                pltpu.VMEM((n_tensor - 1, 3 * rows, 256), bf16),
                *[pltpu.VMEM((rows, units), bf16)] * 2,
                pltpu.VMEM((2, n_z, 2, share, cols), bf16),
                pltpu.VMEM((n_z, 2, share, cols), bf16),
                pltpu.VMEM((n_z, 2, share, cols), bf16),
                pltpu.VMEM((n_z - 1, 2, share, cols), bf16),
                pltpu.SMEM((2,), jnp.int32),
                pltpu.VMEM((1, cols), bf16),
                *[pltpu.SemaphoreType.REGULAR] * 4,
                dma((2,)),
                dma((5, PIECES)),
                *[dma((n, n_tensor - 1))] * 2,
                *[dma((n,))] * 4,
                *[dma((n_z,))] * 2,
                *[dma((n_z - 1,))] * 2,
            ],
            compiler_params=pltpu.CompilerParams(
                collective_id=0, has_side_effects=True, vmem_limit_bytes=48 * 1024 * 1024
            ),
        )(
            *(
                pltpu.with_memory_space_constraint(a, pltpu.HBM)
                for a in (
                    lengths[0, 0], norm_gain, forward_rows[0, 0], saved_rows[0, 0], output_grad[0, 0], down_map[0],
                    up_map[0],
                )
            )
        )
        got_f, got_g, grad_down, grad_up = pl.pallas_call(
            put_out,
            out_shape=tuple(jax.ShapeDtypeStruct(a.shape, a.dtype) for a in results),
            in_specs=[pl.BlockSpec(memory_space=pl.ANY)] * 4,
            out_specs=(in_hbm,) * 4,
            scratch_shapes=[dma((4, PIECES))],
        )(*(pltpu.with_memory_space_constraint(a, pltpu.VMEM) for a in results))
        return got_f[None, None], got_g[None, None], grad_down[None], grad_up[None]

    wide = P("section", "dp", None, "tensor")
    return jax.shard_map(
        shards,
        mesh=mesh,
        in_specs=(
            wide, wide, wide, P("section", "dp", None), P("section", "tensor"),
            P("section", None, "tensor"), P("section", None, "tensor"),
        ),
        out_specs=(wide, wide, P("section", "dp", "tensor"), P("section", "dp", "tensor")),
        check_vma=False,
    )
```
